64 devices in a mesh: rep: 4 (over x, y), dp: 16 (over z, core).
Axes of the slice: x: 2, y: 2, z: 8, core: 2. Of those that a mesh axis runs over, the one named last changes fastest.
The devices are a block of a 4x4x8 slice.
Arguments:
- x: bfloat16 [64, 1024, 768], P(('rep', 'dp')), parts along dimension 0
- dy: bfloat16 [64, 1024, 768], P(('rep', 'dp')), parts along dimension 0
- w_gate: bfloat16 [2, 768, 3072], replicated
- w_up: bfloat16 [2, 768, 3072], replicated
- w_down: bfloat16 [2, 3072, 768], replicated
- m_w_gate: float32 [2, 768, 3072], replicated
- m_w_up: float32 [2, 768, 3072], replicated
- m_w_down: float32 [2, 3072, 768], replicated
- v_w_gate: float32 [2, 768, 3072], replicated
- v_w_up: float32 [2, 768, 3072], replicated
- v_w_down: float32 [2, 3072, 768], replicated
Outputs:
- output 1: bfloat16 [8, 768, 3072], P('rep'), parts along dimension 0
- output 2: bfloat16 [8, 768, 3072], P('rep'), parts along dimension 0
- output 3: bfloat16 [8, 3072, 768], P('rep'), parts along dimension 0
- output 4: float32 [8, 768, 3072], P('rep'), parts along dimension 0
- output 5: float32 [8, 768, 3072], P('rep'), parts along dimension 0
- output 6: float32 [8, 3072, 768], P('rep'), parts along dimension 0
- output 7: float32 [8, 768, 3072], P('rep'), parts along dimension 0
- output 8: float32 [8, 768, 3072], P('rep'), parts along dimension 0
- output 9: float32 [8, 3072, 768], P('rep'), parts along dimension 0
There are 4 independent parts. The reference program is written for one: setup_inputs(seed, part) draws one part's arguments, and reference() takes and returns one part's arrays. A program takes and returns all parts, laid end to end along the dimension named above; an argument that names none is the same for every part.
All inputs are finite; a program needn't handle non-finite values.
Results may differ from the reference program's by a relative error of at most 0.0224.
Values are sent between devices in bfloat16 or wider.
A program may use at most 768 MiB of HBM per device.

```python
import jax
import jax.numpy as jnp
from jax import lax

SEQUENCES = 16
TOKENS = 1024
D = 768
FF = 3072
LAYERS = 2
NAMES = ("w_gate", "w_up", "w_down")
SHAPES = {"w_gate": (LAYERS, D, FF), "w_up": (LAYERS, D, FF), "w_down": (LAYERS, FF, D)}


def bump(key, n, height):
    away = (jnp.arange(n, dtype=jnp.int32) - jax.random.randint(key, (), 0, n, jnp.int32)) % n
    return jnp.where(away < n // 8, height, 1.0)


def together(key, own, strength):
    shared = jax.random.normal(key, own.shape[1:], jnp.float32)
    return (own + strength * shared) * lax.rsqrt(1 + strength * strength)


def setup_inputs(seed: int = 0, part: int = 0) -> dict:
    kx, kdy, ka, kb, kz, kf, kh, kl, *keys = jax.random.split(jax.random.key(seed), 8 + 3 * len(NAMES))
    kx, kdy, ka, kb = (jax.random.fold_in(k, part) for k in (kx, kdy, ka, kb))
    kw, km, kv = (keys[i::3] for i in range(3))
    shape = (SEQUENCES, TOKENS, D)
    much_x, much_dy = jax.random.uniform(kz, (2,), jnp.float32, 0.0, 1.0)
    loud = 2.0 ** jax.random.uniform(jax.random.fold_in(kz, 1), (), jnp.float32, -1.0, 2.0)
    layers = 2.0 ** jax.random.uniform(kl, (LAYERS, 1, 1), jnp.float32, -1.0, 1.0)
    x = together(ka, jax.random.normal(kx, shape, jnp.float32), much_x) * bump(kf, D, 4.0)
    dy = together(kb, jax.random.normal(kdy, shape, jnp.float32), much_dy)
    drawn = {"x": x.astype(jnp.bfloat16), "dy": (loud * dy * (SEQUENCES * TOKENS) ** -0.5).astype(jnp.bfloat16)}
    for key, name in zip(kw, NAMES, strict=True):
        w = jax.random.normal(key, SHAPES[name], jnp.float32) * SHAPES[name][1] ** -0.5
        drawn[name] = (w * {"w_gate": 1.0, "w_up": bump(kh, FF, 4.0), "w_down": layers}[name]).astype(jnp.bfloat16)
    for key, name in zip(km, NAMES, strict=True):
        drawn[f"m_{name}"] = 0.1 * jax.random.normal(key, SHAPES[name], jnp.float32)
    for key, name in zip(kv, NAMES, strict=True):
        drawn[f"v_{name}"] = jax.random.uniform(key, SHAPES[name], jnp.float32, 0.005, 0.015)
    return drawn


def matmul(a, w):
    return jnp.dot(a, w, preferred_element_type=jnp.float32).astype(jnp.bfloat16)


def normed(h):
    wide = h.astype(jnp.float32)
    scale = lax.rsqrt(jnp.mean(wide**2, -1, keepdims=True) + 1e-6)
    return (wide * scale).astype(jnp.bfloat16)


def layer(h, w):
    a = normed(h)
    gate = jnp.dot(a, w["w_gate"], preferred_element_type=jnp.float32)
    up = jnp.dot(a, w["w_up"], preferred_element_type=jnp.float32)
    return h + matmul((jax.nn.silu(gate) * up).astype(jnp.bfloat16), w["w_down"])


def adamw(w, m, v, g):
    m = 0.9 * m + 0.1 * g
    v = 0.95 * v + 0.05 * g * g
    step = m * lax.rsqrt(v + 1e-8) + 0.1 * w
    return (w - 0.02 * step).astype(jnp.bfloat16), m, v


def clipped(gradients, sum_of_squares, count):
    factor = jnp.minimum(1.0, 0.5 * lax.rsqrt(sum_of_squares / count + 1e-30))
    return [g * factor for g in gradients]


def stack(weights, h):
    return lax.scan(lambda h, w: (layer(h, w), None), h, weights)[0]


def reference(x, dy, w_gate, w_up, w_down, m_w_gate, m_w_up, m_w_down, v_w_gate, v_w_up, v_w_down):
    weights = dict(zip(NAMES, (w_gate, w_up, w_down), strict=True))

    def take(so_far, sequence):
        h, by_y = sequence
        _, back = jax.vjp(lambda w: stack(w, h), weights)
        return jax.tree.map(lambda total, term: total + term.astype(jnp.float32), so_far, back(by_y)[0]), None

    none_yet = {name: jnp.zeros(w.shape, jnp.float32) for name, w in weights.items()}
    by_weights, _ = lax.scan(take, none_yet, (x, dy))
    gradients = [by_weights[name].astype(jnp.bfloat16).astype(jnp.float32) for name in NAMES]
    gradients = clipped(gradients, sum(jnp.sum(g * g) for g in gradients), sum(g.size for g in gradients))
    new = [
        adamw(w.astype(jnp.float32), m, v, g)
        for w, m, v, g in zip((w_gate, w_up, w_down), (m_w_gate, m_w_up, m_w_down), (v_w_gate, v_w_up, v_w_down), gradients, strict=True)
    ]
    return tuple(one[which] for which in range(3) for one in new)
```

```python
import functools

import jax
import jax.numpy as jnp
import numpy as np
from jax import lax
from jax.experimental import pallas as pl
from jax.experimental.pallas import tpu as pltpu
from jax.sharding import PartitionSpec as P

F32, BF16 = jnp.float32, jnp.bfloat16
MESH = pl.DeviceIdType.MESH
AHEAD = 3


def dot(a, b, contract):
    return lax.dot_general(a, b, ((contract[:1], contract[1:]), ((), ())), preferred_element_type=F32)


def normed(h):
    wide = h.astype(F32)
    scale = lax.rsqrt(jnp.mean(wide**2, -1, keepdims=True) + 1e-6)
    return (wide * scale).astype(BF16)


def product(gate, up):
    return (jax.nn.silu(gate) * up).astype(BF16)


def reduce_scatter_body(nz, count, *refs):
    lefts, rights = refs[:4], refs[4:10]
    shard, factor = refs[10:12]
    (left, right, ring, other, theirs, own, squares, parts) = refs[12:20]
    (left_sem, right_sem, ring_send, ring_recv, other_send, other_recv, part_send, part_recv) = refs[20:]
    half, width = ring.shape[2:]
    me = lax.axis_index("dp")
    z, c = me // 2, me % 2
    sibling = 2 * z + (1 - c)
    group = 2 * nz
    items = 6 * nz

    for k in range(4):
        pltpu.make_async_copy(lefts[k], left.at[k], left_sem.at[k]).start()

    def fetch(j):
        s, m = j // 6, j % 6
        d = m % 2
        chunk = (z + (2 * d - 1) * (1 + s) + 2 * nz) % nz
        columns = pl.ds(pl.multiple_of(chunk * width, width), width)
        for number in range(6):

            @pl.when(m == number)
            def _():
                pltpu.make_async_copy(rights[number].at[:, columns], right.at[j % 3], right_sem.at[j % 3]).start()

    fetch(0)
    barrier = pltpu.get_barrier_semaphore()
    for i in range(1, group):
        pl.semaphore_signal(barrier, inc=1, device_id={"dp": (me + i) % group}, device_id_type=MESH)
    pl.semaphore_wait(barrier, group - 1)
    for k in range(4):
        pltpu.make_async_copy(lefts[k], left.at[k], left_sem.at[k]).wait()
    squares[...] = jnp.zeros_like(squares)

    def to_sibling(j):
        return pltpu.make_async_remote_copy(
            src_ref=other.at[j % 4],
            dst_ref=theirs.at[j % 6, j // 6],
            send_sem=other_send.at[j % 4],
            recv_sem=other_recv.at[j % 6, j // 6],
            device_id={"dp": sibling},
            device_id_type=MESH,
        )

    def onward(s, m):
        to = (z + 1 - 2 * (m % 2) + nz) % nz
        return pltpu.make_async_remote_copy(
            src_ref=ring.at[m, s],
            dst_ref=ring.at[m, s + 1],
            send_sem=ring_send.at[m, s],
            recv_sem=ring_recv.at[m, s + 1],
            device_id={"dp": 2 * to + c},
            device_id_type=MESH,
        )

    def step(j, carry):
        @pl.when(j < items)
        def _():
            @pl.when(j + 1 < items)
            def _():
                fetch(j + 1)

            m = j % 6
            k, d = m // 2, m % 2
            which = 2 * d + 1 - (k + 1) // 2
            pltpu.make_async_copy(rights[0].at[:, pl.ds(0, width)], right.at[j % 3], right_sem.at[j % 3]).wait()
            columns = right[j % 3]
            away = left[which, pl.ds(pl.multiple_of((1 - c) * half, half), half), :]
            given = jnp.dot(away, columns, preferred_element_type=F32).astype(BF16)

            @pl.when(j >= 4)
            def _():
                to_sibling(j - 4).wait_send()

            other[j % 4] = given
            to_sibling(j).start()
            here = left[which, pl.ds(pl.multiple_of(c * half, half), half), :]
            own[j % 4] = jnp.dot(here, columns, preferred_element_type=F32)

        @pl.when(j >= AHEAD)
        def _():
            i = j - AHEAD
            s, m = i // 6, i % 6
            to_sibling(i).wait_recv()
            own[i % 4] += theirs[m, s].astype(F32)

            @pl.when(s == 0)
            def _():
                ring[m, s] = own[i % 4].astype(BF16)
                onward(s, m).start()

            @pl.when((s > 0) & (s < nz - 1))
            def _():
                onward(s - 1, m).wait_recv()
                ring[m, s] = (own[i % 4] + ring[m, s].astype(F32)).astype(BF16)
                onward(s, m).start()

            @pl.when(s == nz - 1)
            def _():
                onward(s - 1, m).wait_recv()
                total = (own[i % 4] + ring[m, s].astype(F32)).astype(BF16)
                wide = total.astype(F32)
                square = jnp.sum((wide * wide).reshape(half // 8, 8, width), axis=0)
                squares[...] += sum(square[:, at : at + 128] for at in range(0, width, 128))
                place = (1 - m % 2) * 3 + (m // 2 + 2) % 3

                @pl.when(m < 2)
                def _():
                    shard[place] = wide.T.astype(BF16)

                @pl.when(m >= 2)
                def _():
                    shard[place] = total

        return carry

    lax.fori_loop(0, items + AHEAD, step, 0)
    for i in range(items - 4, items):
        to_sibling(i).wait_send()
    for m in range(6):
        for s in range(nz - 1):
            onward(s, m).wait_send()

    parts[me] = squares[...]

    def part(i):
        return pltpu.make_async_remote_copy(
            src_ref=parts.at[me],
            dst_ref=parts.at[me],
            send_sem=part_send.at[i],
            recv_sem=part_recv.at[me],
            device_id={"dp": (me + i) % group},
            device_id_type=MESH,
        )

    for i in range(1, group):
        part(i).start()
    for i in range(1, group):
        part(i).wait_send()
    for i in range(1, group):
        source = (me + i) % group
        pltpu.make_async_copy(parts.at[source], parts.at[source], part_recv.at[source]).wait()
    total = jnp.sum(jnp.sum(parts[...], axis=0))
    factor[...] = jnp.minimum(1.0, 0.5 * lax.rsqrt(jnp.full(factor.shape, total, F32) / count + 1e-30))


def reduce_scatter(lefts, rights, nz, count):
    d, tokens = lefts[0].shape
    half, width = d // 2, rights[0].shape[1] // nz
    assert half == width
    vmem, dma = pltpu.VMEM, pltpu.SemaphoreType.DMA
    flops = 2 * 6 * d * tokens * width * nz
    return pl.pallas_call(
        functools.partial(reduce_scatter_body, nz, count),
        in_specs=[pl.BlockSpec(memory_space=pl.ANY)] * 10,
        out_specs=[pl.BlockSpec(memory_space=pltpu.VMEM)] * 2,
        out_shape=[jax.ShapeDtypeStruct((6, half, width), BF16), jax.ShapeDtypeStruct((8, 128), F32)],
        scratch_shapes=[
            vmem((4, d, tokens), BF16),
            vmem((3, tokens, width), BF16),
            vmem((6, nz, half, width), BF16),
            vmem((4, half, width), BF16),
            vmem((6, nz, half, width), BF16),
            vmem((4, half, width), F32),
            vmem((8, 128), F32),
            vmem((2 * nz, 8, 128), F32),
            dma((4,)),
            dma((3,)),
            dma((6, nz)),
            dma((6, nz)),
            dma((4,)),
            dma((6, nz)),
            dma((2 * nz,)),
            dma((2 * nz,)),
        ],
        compiler_params=pltpu.CompilerParams(collective_id=0, has_side_effects=True, vmem_limit_bytes=62 << 20),
        cost_estimate=pl.CostEstimate(flops=flops, bytes_accessed=6 * tokens * width * nz * 2, transcendentals=0),
        name="reduce_scatter",
    )(*lefts, *rights)


def adamw_body(units, arrays, pos, factor, *refs):
    gs, olds, news, token = refs[:arrays], refs[arrays : arrays + 9], refs[-10:-1], refs[-1]
    u = pl.program_id(0)
    token[...] = factor[...]
    for number in range(arrays):
        mine = [i for i, unit in enumerate(units) if unit[0] == number]

        @pl.when((u >= mine[0]) & (u <= mine[-1]))
        def _():
            for i in range(3):
                w, m, v = olds[i], olds[3 + i], olds[6 + i]
                grad = gs[number][i].astype(F32) * factor[0:1, 0:1]
                m_new = 0.9 * m[0] + 0.1 * grad
                v_new = 0.95 * v[0] + 0.05 * grad * grad
                wide = w[0].astype(F32)
                move = m_new * lax.rsqrt(v_new + 1e-8) + 0.1 * wide
                news[i][0] = (wide - 0.02 * move).astype(BF16)
                news[3 + i][0] = m_new
                news[6 + i][0] = v_new


def adamw(factor, gs, units, pos, offset, olds, so_far, cut=2):
    side = gs[0].shape[1]
    rows = side // cut

    def g_spec(number):
        mine = [i for i, unit in enumerate(units) if unit[0] == number]
        first, last = mine[0], mine[-1]
        start = units[first][2]

        def index(u, q, pos):
            at = jnp.clip(u, first, last)
            return (start + at - first, jnp.where(u < first, 0, jnp.where(u > last, cut - 1, q)), 0)

        return pl.BlockSpec((3, rows, side), index)

    assert all(unit[1] == i % 2 for i, unit in enumerate(units))
    wide = pl.BlockSpec((1, rows, side), lambda u, q, pos: (u % 2, pos[offset + u, 1] * cut + q, pos[offset + u, 0]))
    tall = pl.BlockSpec((1, rows, side), lambda u, q, pos: (u % 2, pos[offset + u, 0] * cut + q, pos[offset + u, 1]))
    specs = [wide, wide, tall] * 3
    aliased = [] if so_far is None else list(so_far)
    n = len(units) * 3 * side * side
    return pl.pallas_call(
        functools.partial(adamw_body, units, len(gs)),
        grid_spec=pltpu.PrefetchScalarGridSpec(
            num_scalar_prefetch=1,
            grid=(len(units), cut),
            in_specs=[pl.BlockSpec((8, 128), lambda u, q, pos: (0, 0))]
            + [g_spec(number) for number in range(len(gs))]
            + specs
            + [pl.BlockSpec(memory_space=pl.ANY)] * len(aliased),
            out_specs=specs + [pl.BlockSpec((8, 128), lambda u, q, pos: (0, 0))],
        ),
        out_shape=[jax.ShapeDtypeStruct(o.shape, o.dtype) for o in olds] + [jax.ShapeDtypeStruct((8, 128), F32)],
        input_output_aliases={2 + len(gs) + 9 + i: i for i in range(len(aliased))},
        compiler_params=pltpu.CompilerParams(vmem_limit_bytes=60 << 20),
        cost_estimate=pl.CostEstimate(flops=500 * n, bytes_accessed=22 * n, transcendentals=n),
        name="adamw",
    )(pos, factor, *gs, *olds, *aliased)


def after(token, *held):
    return pl.pallas_call(
        lambda *refs: None,
        in_specs=[pl.BlockSpec(memory_space=pl.ANY)] * (1 + len(held)),
        out_specs=[pl.BlockSpec(memory_space=pl.ANY)] * len(held),
        out_shape=[jax.ShapeDtypeStruct(a.shape, a.dtype) for a in held],
        input_output_aliases={1 + i: i for i in range(len(held))},
        compiler_params=pltpu.CompilerParams(has_side_effects=True),
        name="after",
    )(token, *held)


def solution(mesh):
    group = mesh.shape["dp"]
    nz = group // 2

    def step(x, dy, *arrays):
        weights = arrays[:3]
        layers = weights[0].shape[0]
        assert layers == 2 and nz % 2 == 0
        w_gate, w_up, w_down = ([w[n] for n in range(layers)] for w in weights)
        h, kept = x[0], []
        for n in range(layers):
            a = normed(h)
            gate, up = dot(a, w_gate[n], (1, 0)), dot(a, w_up[n], (1, 0))
            hid = product(gate, up)
            kept.append((h, a, gate, up, hid))
            if n < layers - 1:
                h = h + dot(hid, w_down[n], (1, 0)).astype(BF16)
        by_h, pairs = dy[0], {}
        for n in reversed(range(layers)):
            h, a, gate, up, hid = kept[n]
            by_hid = dot(by_h, w_down[n], (1, 1)).astype(BF16)
            _, back = jax.vjp(product, gate, up)
            by_gate, by_up = (t.astype(BF16) for t in back(by_hid))
            pairs[n] = (a.T, by_h.T, hid, by_gate, by_up)
            if n:
                by_a = dot(by_gate, w_gate[n], (1, 1)).astype(BF16) + dot(by_up, w_up[n], (1, 1)).astype(BF16)
                _, back = jax.vjp(normed, h)
                by_h = by_h + back(by_a)[0]
        lefts = [pairs[1][0], pairs[1][1], pairs[0][0], pairs[0][1]]
        rights = [pairs[1 - m % 2][2 + m // 2] for m in range(6)]
        own, factor = reduce_scatter(lefts, rights, nz, float(sum(w.size for w in weights)))

        up_ring = [(2 * z + c, 2 * ((z + 1) % nz) + c) for z in range(nz) for c in range(2)]
        down_ring = [(b, a) for a, b in up_ring]
        across = [(i, i ^ 1) for i in range(group)]
        both = lambda i: [(i, 0, 0), (i, 1, 1)]
        far = nz // 2
        near = [(0, True), (0, False)]
        rounds = [near] + [[(-r, True), (r, True), (-r, False), (r, False)] for r in range(1, far + 1)]
        table = [
            [((i // 2 + dz) % nz, i % 2 if same else 1 - i % 2) for r, places in enumerate(rounds) for dz, same in places for _ in range(2 if r < far else 1)]
            for i in range(group)
        ]
        pos = lax.dynamic_index_in_dim(jnp.asarray(np.array(table, np.int32)), lax.axis_index("dp"), 0, keepdims=False)

        rise, fall, new, offset = own, own, None, 0
        here = [own]
        for r in range(far):
            if r < far - 1:
                next_rise, next_fall = lax.ppermute(rise, "dp", up_ring), lax.ppermute(fall, "dp", down_ring)
            else:
                next_rise, next_fall = lax.ppermute(rise[:3], "dp", up_ring), lax.ppermute(fall[3:], "dp", down_ring)
            gs = here + [lax.ppermute(g, "dp", across) for g in here]
            units = [unit for i in range(len(gs)) for unit in both(i)]
            *new, token = adamw(factor, gs, units, pos, offset, arrays, new)
            offset += len(units)
            rise, fall = after(token, next_rise, next_fall)
            here = [rise, fall]
        gs = here + [lax.ppermute(g, "dp", across) for g in here]
        *new, token = adamw(factor, gs, [(0, 0, 0), (1, 1, 0), (2, 0, 0), (3, 1, 0)], pos, offset, arrays, new)
        return tuple(new)

    return jax.shard_map(
        step,
        mesh=mesh,
        in_specs=(P(("rep", "dp"), None, None),) * 2 + (P(None, None, None),) * 9,
        out_specs=(P("rep", None, None),) * 9,
        check_vma=False,
    )
```

```python
import functools

import jax
import jax.numpy as jnp
import numpy as np
from jax import lax
from jax.experimental import pallas as pl
from jax.experimental.pallas import tpu as pltpu
from jax.sharding import PartitionSpec as P

F32, BF16 = jnp.float32, jnp.bfloat16
MESH = pl.DeviceIdType.MESH
AHEAD = 3


def dot(a, b, contract):
    return lax.dot_general(a, b, ((contract[:1], contract[1:]), ((), ())), preferred_element_type=F32)


def passes_body(nb, x, dy, w_gate, w_up, w_down, at1, dyt, at0, dht, hid1, gate1, up1, hid0, gate0, up0, wg, wu, wd, kept_gate, kept_up, sem):
    copies = [
        pltpu.make_async_copy(src.at[n], dst.at[n], sem.at[3 * n + i])
        for n in range(2)
        for i, (src, dst) in enumerate(((w_gate, wg), (w_up, wu), (w_down, wd)))
    ]
    first = pl.program_id(0) == 0

    def arrived(*which):
        @pl.when(first)
        def _():
            for i in which:
                copies[i].wait()

    @pl.when(first)
    def _():
        for copy in copies:
            copy.start()

    ff = wg.shape[2]
    cut = ff // nb

    def columns(i):
        return pl.ds(pl.multiple_of(i * cut, cut), cut)

    def turn(a):
        return a.astype(F32).T.astype(BF16)

    def norm(h):
        wide = h.astype(F32)
        scale = lax.rsqrt(jnp.mean(wide**2, -1, keepdims=True) + 1e-6)
        return wide, scale, (wide * scale).astype(BF16)

    def by_product(gate, up, ct):
        s = jax.nn.sigmoid(gate)
        silu = gate * s
        by_silu = ct * up
        return (by_silu * (s + silu * (1.0 - s))).astype(BF16), (ct * silu).astype(BF16), silu

    h = x[0]
    _, _, a0 = norm(h)
    at0[...] = turn(a0)
    ct = dy[0]
    dyt[...] = turn(ct)

    arrived(0, 1)

    def forward(i, carry):
        at = columns(i)
        gate = jnp.dot(a0, wg[0, :, at], preferred_element_type=F32)
        up = jnp.dot(a0, wu[0, :, at], preferred_element_type=F32)
        kept_gate[:, at] = gate
        kept_up[:, at] = up
        hid0[:, at] = (gate * jax.nn.sigmoid(gate) * up).astype(BF16)
        return carry

    lax.fori_loop(0, nb, forward, 0, unroll=2)
    arrived(2)
    h = h + jnp.dot(hid0[...], wd[0], preferred_element_type=F32).astype(BF16)
    wide, scale, a1 = norm(h)
    at1[...] = turn(a1)
    arrived(3, 4, 5)

    def backward(i, carry):
        at = columns(i)
        gate = jnp.dot(a1, wg[1, :, at], preferred_element_type=F32)
        up = jnp.dot(a1, wu[1, :, at], preferred_element_type=F32)
        by_hid = dot(ct, wd[1, at, :], (1, 1)).astype(BF16).astype(F32)
        by_gate, by_up, silu = by_product(gate, up, by_hid)
        gate1[:, at] = by_gate
        up1[:, at] = by_up
        hid1[:, at] = (silu * up).astype(BF16)
        return carry

    lax.fori_loop(0, nb, backward, 0, unroll=2)
    by_a = dot(gate1[...], wg[1], (1, 1)).astype(BF16) + dot(up1[...], wu[1], (1, 1)).astype(BF16)
    by_a = by_a.astype(F32)
    by_scale = jnp.sum(by_a * wide, -1, keepdims=True)
    by_h = by_a * scale - wide * (by_scale * scale * scale * scale / wide.shape[1])
    ct = ct + by_h.astype(BF16)
    dht[...] = turn(ct)

    def last(i, carry):
        at = columns(i)
        by_hid = dot(ct, wd[0, at, :], (1, 1)).astype(BF16).astype(F32)
        by_gate, by_up, _ = by_product(kept_gate[:, at], kept_up[:, at], by_hid)
        gate0[:, at] = by_gate
        up0[:, at] = by_up
        return carry

    lax.fori_loop(0, nb, last, 0, unroll=2)


def passes(x, dy, w_gate, w_up, w_down, block=256, nb=3):
    _, tokens, d = x.shape
    ff = w_gate.shape[2]
    rows = pl.BlockSpec((1, block, d), lambda i: (0, i, 0))
    turned = pl.BlockSpec((d, block), lambda i: (0, i))
    long = pl.BlockSpec((block, ff), lambda i: (i, 0))
    vmem = pltpu.VMEM
    return pl.pallas_call(
        functools.partial(passes_body, nb),
        grid=(tokens // block,),
        in_specs=[rows, rows] + [pl.BlockSpec(memory_space=pl.ANY)] * 3,
        out_specs=[turned] * 4 + [long] * 6,
        out_shape=[jax.ShapeDtypeStruct((d, tokens), BF16)] * 4 + [jax.ShapeDtypeStruct((tokens, ff), BF16)] * 6,
        scratch_shapes=[
            vmem(w_gate.shape, BF16),
            vmem(w_up.shape, BF16),
            vmem(w_down.shape, BF16),
            vmem((block, ff), F32),
            vmem((block, ff), F32),
            pltpu.SemaphoreType.DMA((6,)),
        ],
        compiler_params=pltpu.CompilerParams(vmem_limit_bytes=67000000),
        cost_estimate=pl.CostEstimate(flops=2 * 9 * tokens * d * ff, bytes_accessed=6 * d * ff * 2 + 6 * tokens * ff * 2, transcendentals=0),
        name="passes",
    )(x, dy, w_gate, w_up, w_down)


def reduce_scatter_body(nz, count, *refs):
    lefts, rights = refs[:4], refs[4:10]
    shards, factor = refs[10:12], refs[12]
    (left, right, ring, other, theirs, own, squares, parts) = refs[13:21]
    (left_sem, right_sem, ring_send, ring_recv, other_send, other_recv, part_send, part_recv) = refs[21:]
    half, width = ring.shape[2:]
    me = lax.axis_index("dp")
    z, c = me // 2, me % 2
    sibling = 2 * z + (1 - c)
    group = 2 * nz
    items = 6 * nz

    for k in range(4):
        pltpu.make_async_copy(lefts[k], left.at[k], left_sem.at[k]).start()

    def fetch(j):
        s, m = j // 6, j % 6
        d = m % 2
        chunk = (z + (2 * d - 1) * (1 + s) + 2 * nz) % nz
        columns = pl.ds(pl.multiple_of(chunk * width, width), width)
        for number in range(6):

            @pl.when(m == number)
            def _():
                pltpu.make_async_copy(rights[number].at[:, columns], right.at[j % 3], right_sem.at[j % 3]).start()

    fetch(0)
    barrier = pltpu.get_barrier_semaphore()
    for i in range(1, group):
        pl.semaphore_signal(barrier, inc=1, device_id={"dp": (me + i) % group}, device_id_type=MESH)
    pl.semaphore_wait(barrier, group - 1)
    for k in range(4):
        pltpu.make_async_copy(lefts[k], left.at[k], left_sem.at[k]).wait()
    squares[...] = jnp.zeros_like(squares)

    def to_sibling(j):
        return pltpu.make_async_remote_copy(
            src_ref=other.at[j % 4],
            dst_ref=theirs.at[j % 6, j // 6],
            send_sem=other_send.at[j % 4],
            recv_sem=other_recv.at[j % 6, j // 6],
            device_id={"dp": sibling},
            device_id_type=MESH,
        )

    def onward(s, m):
        to = (z + 1 - 2 * (m % 2) + nz) % nz
        return pltpu.make_async_remote_copy(
            src_ref=ring.at[m, s],
            dst_ref=ring.at[m, s + 1],
            send_sem=ring_send.at[m, s],
            recv_sem=ring_recv.at[m, s + 1],
            device_id={"dp": 2 * to + c},
            device_id_type=MESH,
        )

    def step(j, carry):
        @pl.when(j < items)
        def _():
            @pl.when(j + 1 < items)
            def _():
                fetch(j + 1)

            m = j % 6
            k, d = m // 2, m % 2
            which = 2 * d + 1 - (k + 1) // 2
            pltpu.make_async_copy(rights[0].at[:, pl.ds(0, width)], right.at[j % 3], right_sem.at[j % 3]).wait()
            columns = right[j % 3]
            away = left[which, pl.ds(pl.multiple_of((1 - c) * half, half), half), :]
            given = jnp.dot(away, columns, preferred_element_type=F32).astype(BF16)

            @pl.when(j >= 4)
            def _():
                to_sibling(j - 4).wait_send()

            other[j % 4] = given
            to_sibling(j).start()
            here = left[which, pl.ds(pl.multiple_of(c * half, half), half), :]
            own[j % 4] = jnp.dot(here, columns, preferred_element_type=F32)

        @pl.when(j >= AHEAD)
        def _():
            i = j - AHEAD
            s, m = i // 6, i % 6
            to_sibling(i).wait_recv()
            own[i % 4] += theirs[m, s].astype(F32)

            @pl.when(s == 0)
            def _():
                ring[m, s] = own[i % 4].astype(BF16)
                onward(s, m).start()

            @pl.when((s > 0) & (s < nz - 1))
            def _():
                onward(s - 1, m).wait_recv()
                ring[m, s] = (own[i % 4] + ring[m, s].astype(F32)).astype(BF16)
                onward(s, m).start()

            @pl.when(s == nz - 1)
            def _():
                onward(s - 1, m).wait_recv()
                total = (own[i % 4] + ring[m, s].astype(F32)).astype(BF16)
                wide = total.astype(F32)
                square = jnp.sum((wide * wide).reshape(half // 8, 8, width), axis=0)
                squares[...] += sum(square[:, at : at + 128] for at in range(0, width, 128))
                for d in range(2):

                    @pl.when(m == d)
                    def _():
                        shards[d][2] = wide.T.astype(BF16)

                    @pl.when((m >= 2) & (m % 2 == d))
                    def _():
                        shards[d][m // 2 - 1] = total

        return carry

    lax.fori_loop(0, items + AHEAD, step, 0)
    for i in range(items - 4, items):
        to_sibling(i).wait_send()
    for m in range(6):
        for s in range(nz - 1):
            onward(s, m).wait_send()

    parts[me] = squares[...]

    def part(i):
        return pltpu.make_async_remote_copy(
            src_ref=parts.at[me],
            dst_ref=parts.at[me],
            send_sem=part_send.at[i],
            recv_sem=part_recv.at[me],
            device_id={"dp": (me + i) % group},
            device_id_type=MESH,
        )

    for i in range(1, group):
        part(i).start()
    for i in range(1, group):
        part(i).wait_send()
    for i in range(1, group):
        source = (me + i) % group
        pltpu.make_async_copy(parts.at[source], parts.at[source], part_recv.at[source]).wait()
    total = jnp.sum(jnp.sum(parts[...], axis=0))
    factor[...] = jnp.minimum(1.0, 0.5 * lax.rsqrt(jnp.full(factor.shape, total, F32) / count + 1e-30))


def reduce_scatter(lefts, rights, nz, count):
    d, tokens = lefts[0].shape
    half, width = d // 2, rights[0].shape[1] // nz
    assert half == width
    vmem, dma = pltpu.VMEM, pltpu.SemaphoreType.DMA
    flops = 2 * 6 * d * tokens * width * nz
    return pl.pallas_call(
        functools.partial(reduce_scatter_body, nz, count),
        in_specs=[pl.BlockSpec(memory_space=pl.ANY)] * 10,
        out_specs=[pl.BlockSpec(memory_space=pltpu.VMEM)] * 3,
        out_shape=[jax.ShapeDtypeStruct((3, half, width), BF16)] * 2 + [jax.ShapeDtypeStruct((8, 128), F32)],
        scratch_shapes=[
            vmem((4, d, tokens), BF16),
            vmem((3, tokens, width), BF16),
            vmem((6, nz, half, width), BF16),
            vmem((4, half, width), BF16),
            vmem((6, nz, half, width), BF16),
            vmem((4, half, width), F32),
            vmem((8, 128), F32),
            vmem((2 * nz, 8, 128), F32),
            dma((4,)),
            dma((3,)),
            dma((6, nz)),
            dma((6, nz)),
            dma((4,)),
            dma((6, nz)),
            dma((2 * nz,)),
            dma((2 * nz,)),
        ],
        compiler_params=pltpu.CompilerParams(collective_id=0, has_side_effects=True, vmem_limit_bytes=62 << 20),
        cost_estimate=pl.CostEstimate(flops=flops, bytes_accessed=6 * tokens * width * nz * 2, transcendentals=0),
        name="reduce_scatter",
    )(*lefts, *rights)


def adamw_body(units, pos, factor, *refs):
    gs, olds, news, token = refs[:units], refs[units : units + 9], refs[-10:-1], refs[-1]
    u = pl.program_id(0)
    some = olds[0].shape[1] // 4
    token[...] = factor[...]
    for number in range(units):

        @pl.when(u == number)
        def _():
            def part(j, carry):
                at = pl.ds(pl.multiple_of(j * some, some), some)
                for i in range(3):
                    w, m, v = olds[i], olds[3 + i], olds[6 + i]
                    grad = gs[number][i, at, :].astype(F32) * factor[0:1, 0:1]
                    m_new = 0.9 * m[0, at, :] + 0.1 * grad
                    v_new = 0.95 * v[0, at, :] + 0.05 * grad * grad
                    wide = w[0, at, :].astype(F32)
                    move = m_new * lax.rsqrt(v_new + 1e-8) + 0.1 * wide
                    news[i][0, at, :] = (wide - 0.02 * move).astype(BF16)
                    news[3 + i][0, at, :] = m_new
                    news[6 + i][0, at, :] = v_new
                return carry

            lax.fori_loop(0, 4, part, 0)


def adamw(factor, gs, pos, offset, olds, so_far, cut=2):
    units, side = len(gs), gs[0].shape[1]
    rows = side // cut

    def g_spec(number):
        return pl.BlockSpec((3, rows, side), lambda u, q, pos: (0, jnp.where(u < number, 0, jnp.where(u > number, cut - 1, q)), 0))

    wide = lambda u, q, pos: (pos[offset + u, 2], pos[offset + u, 1] * cut + q, pos[offset + u, 0])
    tall = lambda u, q, pos: (pos[offset + u, 2], pos[offset + u, 0] * cut + q, pos[offset + u, 1])
    specs = [pl.BlockSpec((1, rows, side), index) for index in (wide, wide, tall)] * 3
    aliased = [] if so_far is None else list(so_far)
    n = units * 3 * side * side
    return pl.pallas_call(
        functools.partial(adamw_body, units),
        grid_spec=pltpu.PrefetchScalarGridSpec(
            num_scalar_prefetch=1,
            grid=(units, cut),
            in_specs=[pl.BlockSpec((8, 128), lambda u, q, pos: (0, 0))]
            + [g_spec(number) for number in range(units)]
            + specs
            + [pl.BlockSpec(memory_space=pl.ANY)] * len(aliased),
            out_specs=specs + [pl.BlockSpec((8, 128), lambda u, q, pos: (0, 0))],
        ),
        out_shape=[jax.ShapeDtypeStruct(o.shape, o.dtype) for o in olds] + [jax.ShapeDtypeStruct((8, 128), F32)],
        input_output_aliases={2 + units + 9 + i: i for i in range(len(aliased))},
        compiler_params=pltpu.CompilerParams(vmem_limit_bytes=67000000),
        cost_estimate=pl.CostEstimate(flops=500 * n, bytes_accessed=22 * n, transcendentals=n),
        name="adamw",
    )(pos, factor, *gs, *olds, *aliased)


def after(token, *held):
    return pl.pallas_call(
        lambda *refs: None,
        in_specs=[pl.BlockSpec(memory_space=pl.ANY)] * (1 + len(held)),
        out_specs=[pl.BlockSpec(memory_space=pl.ANY)] * len(held),
        out_shape=[jax.ShapeDtypeStruct(a.shape, a.dtype) for a in held],
        input_output_aliases={1 + i: i for i in range(len(held))},
        compiler_params=pltpu.CompilerParams(has_side_effects=True),
        name="after",
    )(token, *held)


def solution(mesh):
    group = mesh.shape["dp"]
    nz = group // 2

    def step(x, dy, *arrays):
        weights = arrays[:3]
        layers = weights[0].shape[0]
        assert layers == 2 and nz % 2 == 0
        *lefts, hid1, gate1, up1, hid0, gate0, up0 = passes(x, dy, *weights)
        rights = [hid1, hid0, gate1, gate0, up1, up0]
        own1, own0, factor = reduce_scatter(lefts, rights, nz, float(sum(w.size for w in weights)))

        up_ring = [(2 * z + c, 2 * ((z + 1) % nz) + c) for z in range(nz) for c in range(2)]
        down_ring = [(b, a) for a, b in up_ring]
        rise = lambda a: lax.ppermute(a, "dp", up_ring)
        fall = lambda a: lax.ppermute(a, "dp", down_ring)
        across = lambda a: lax.ppermute(a, "dp", [(i, i ^ 1) for i in range(group)])
        far = nz // 2
        pieces = [((0, 1), (0, 0))] + [((r, layer), (-r, layer)) for r in range(1, far) for layer in (1, 0)] + [((far, 0), (far, 1))]
        turns = [[(*p, True) for p in pieces[0]]]
        for before, now in zip(pieces, pieces[1:], strict=False):
            turns.append([(*p, True) for p in now] + [(*p, False) for p in before])
        turns.append([(*p, False) for p in pieces[-1]])
        table = [[((i // 2 - r) % nz, i % 2 if same else 1 - i % 2, layer) for turn in turns for r, layer, same in turn] for i in range(group)]
        pos = lax.dynamic_index_in_dim(jnp.asarray(np.array(table, np.int32)), lax.axis_index("dp"), 0, keepdims=False)

        coming = [(rise(own1), fall(own1)), (rise(own0), fall(own0))]
        near, beside = [own1, own0], []
        new, offset = None, 0
        for turn in range(len(pieces)):
            gs = near + beside
            beside = [across(g) for g in near]
            *new, token = adamw(factor, gs, pos, offset, arrays, new)
            offset += len(gs)
            if turn + 1 < len(pieces):
                near = list(after(token, *coming[turn]))
                if turn + 3 < len(pieces) - 1:
                    coming.append((rise(near[0]), fall(near[1])))
                elif turn + 3 == len(pieces) - 1:
                    last_fall = fall(near[1])
                elif turn + 3 == len(pieces):
                    coming.append((rise(near[0]), last_fall))
        *new, token = adamw(factor, beside, pos, offset, arrays, new)
        return tuple(new)

    return jax.shard_map(
        step,
        mesh=mesh,
        in_specs=(P(("rep", "dp"), None, None),) * 2 + (P(None, None, None),) * 9,
        out_specs=(P("rep", None, None),) * 9,
        check_vma=False,
    )
```
